32 devices in a mesh: dp: 4 (over z), section: 4 (over x, core), head: 2 (over y).
Axes of the slice: x: 2, y: 2, z: 4, core: 2. Of those that a mesh axis runs over, the one named last changes fastest.
Arguments:
- q_latent: bfloat16 [4, 2048, 1536], P('section', 'dp'), may hold values from -6 to 6
- kv_latent: bfloat16 [4, 2048, 576], P('section', 'dp'), may hold values from -6 to 6
- segment_ids: int32 [2048], P('dp'), may hold values from 0 to 31, never falling along the last dimension, each value on 1 to 512 neighbouring positions
- q_weight: bfloat16 [4, 1536, 12288], P('section', 'dp', 'head'), may hold values from -100 to 100
- k_weight: bfloat16 [4, 512, 8192], P('section', None, 'head'), may hold values from -0.25 to 0.25
Outputs:
- logit_ratio: float32 [4, 64], P(None, 'head')
- scaled_q: bfloat16 [4, 1536, 12288], P('section', 'dp', 'head')
- scaled_k: bfloat16 [4, 512, 8192], P('section', None, 'head')
The draws below stay inside these ranges and needn't reach their ends.
All inputs are finite; a program needn't handle non-finite values.
Results may differ from the reference program's by a relative error of at most 0.0034.
Values may be sent and summed in bfloat16 or wider, within the bound.
A program may use at most 128 MiB of HBM per device.

```python
import math
import jax
import jax.numpy as jnp
import numpy as np
from jax import lax

D_Q = 1536
D_KV = 512
NOPE = 128
ROPE = 64
HEADS = 64
SEQ = 512
LAYERS = 4
TOKENS = 2048
N_DP = 4


def draw_q_weight(key, part):
    scale_key, entry_key = jax.random.split(jax.random.fold_in(key, 11))
    head_scale = jnp.exp(jax.random.uniform(scale_key, (LAYERS, 1, HEADS, 1), jnp.float32, math.log(2.0), math.log(100.0)))
    entries = jax.random.normal(entry_key, (LAYERS, D_Q, HEADS, NOPE + ROPE), jnp.float32)
    weights = entries * head_scale / math.sqrt(D_Q)
    return weights.reshape(LAYERS, D_Q, HEADS * (NOPE + ROPE)).astype(jnp.bfloat16)


def level_of(stream_key, dims, cuts, smallest, top_value):
    def one(dim, blocks):
        steps = jax.random.uniform(jax.random.fold_in(jax.random.fold_in(stream_key, 6), dim), (blocks,), jnp.float32, smallest / len(cuts), top_value / len(cuts))
        return jnp.repeat(jnp.exp(steps), dims[dim] // blocks).reshape((-1,) + (1,) * (len(dims) - dim - 1))

    loudness = one(*cuts[0])
    for cut in cuts[1:]:
        loudness = loudness * one(*cut)
    return loudness


def split_up(amount, total, limit, slope):
    loads = [(1 << 20) // math.isqrt(standing ** slope) + 1 for standing in range(2, amount + 1)]
    rest, counts = total - limit - (amount - 1), [1] * (amount - 1)
    while rest > 0:
        free = [i for i in range(amount - 1) if counts[i] < limit]
        mass, remaining = sum([loads[i] for i in free]), rest
        for i in free:
            extra = min(limit - counts[i], max(1, remaining * loads[i] // mass), rest)
            counts[i] = counts[i] + extra
            rest = rest - extra
    return np.array([limit] + counts)


def ragged_sizes(key, amount, total, limit, skew):
    if amount == 2:
        one = jax.random.randint(key, (), max(1, total - limit), min(limit, total - 1) + 1)
        return jnp.stack([one, total - one])
    lengths = jnp.asarray(split_up(amount, total, limit, skew), jnp.int32)
    pairs = (amount - 1) // 2
    source_of, taker = lengths[1:1 + 2 * pairs:2], lengths[2:2 + 2 * pairs:2]
    margin = jnp.minimum(source_of - 1, limit - taker)
    shifted = jax.random.randint(jax.random.fold_in(key, 1), (pairs,), 0, 1 << 20) % (margin + 1)
    lengths = lengths.at[1:1 + 2 * pairs:2].set(source_of - shifted).at[2:2 + 2 * pairs:2].set(taker + shifted)
    return lengths[jax.random.permutation(jax.random.fold_in(key, 2), amount)]


def gaussian(key, extent, width, reach, cuts=(), kind=jnp.bfloat16):
    values = jax.random.normal(key, extent, jnp.float32) * width
    if len(cuts) > 0:
        values = level_of(key, extent, cuts, -0.22, 0.18) * values
    return jnp.clip(values, min=-reach, max=reach).astype(kind)


def setup_inputs(seed: int = 0) -> dict:
    arg_keys = jax.random.split(jax.random.key(seed), 6)
    return {
        "q_latent": gaussian(arg_keys[0], (LAYERS, TOKENS, D_Q), 1.0, 6.0, ((0, 4), (1, 4))),
        "kv_latent": gaussian(arg_keys[1], (LAYERS, TOKENS, D_KV + ROPE), 1.0, 6.0, ((0, 4), (1, 4))),
        "segment_ids": jnp.searchsorted(jnp.cumsum(ragged_sizes(arg_keys[2], max(4, TOKENS // 64), TOKENS, min(512, TOKENS // 2), 1)), jnp.arange(TOKENS), side="right").astype(jnp.int32),
        "q_weight": draw_q_weight(jax.random.fold_in(arg_keys[5], 71), 0),
        "k_weight": gaussian(arg_keys[4], (LAYERS, D_KV, HEADS * NOPE), D_KV ** -0.5, 0.25, ((0, 4), (2, 2))),
    }


clip_threshold = 100.0
rope_base = 50000.0

def rotate(values, positions):
    half_width = values.shape[-1] // 2
    frequency = rope_base ** (-jnp.arange(half_width, dtype=jnp.float32) / half_width)
    angles = positions[:, None].astype(jnp.float32) * frequency[None, :]
    cosine = jnp.cos(angles)[:, None, :]
    sine_part = jnp.sin(angles)[:, None, :]
    lower_half = values[..., :half_width]
    upper_half = values[..., half_width:]
    return jnp.concatenate([lower_half * cosine - upper_half * sine_part, upper_half * cosine + lower_half * sine_part], -1)

def sequence_maxima(q_full, kv_rows, segments, w_key):
    length = kv_rows.shape[0]
    heads_here = w_key.shape[1] // NOPE
    q_full = q_full.reshape(length, heads_here, NOPE + ROPE)
    positions = jnp.arange(length, dtype=jnp.int32)
    queries = jnp.concatenate([q_full[..., :NOPE], rotate(q_full[..., NOPE:], positions)], -1).astype(jnp.bfloat16)
    key_nope = jnp.dot(kv_rows[:, :D_KV], w_key, preferred_element_type=jnp.float32).astype(jnp.bfloat16)
    key_nope = key_nope.reshape(length, heads_here, NOPE)
    key_rope = jnp.broadcast_to(kv_rows[:, None, D_KV:], (length, heads_here, ROPE))
    keys_all = jnp.concatenate([key_nope, key_rope], -1)
    logits = jnp.einsum('shd,thd->hst', queries.astype(jnp.float32), keys_all.astype(jnp.float32))
    logits = logits * (NOPE + ROPE) ** (-0.5)
    allowed = (segments[:, None] == segments[None, :]) & (positions[None, :] <= positions[:, None])
    return lax.optimization_barrier(jnp.max(jnp.where(allowed[None], logits, -1e+30), axis=(1, 2)))

def scale_weights(own_max, q_weight, k_weight):
    factor = clip_threshold / jnp.maximum(own_max, clip_threshold)
    square_root = jnp.sqrt(factor)
    layers_here, heads_here = own_max.shape
    column_scale = jnp.concatenate([jnp.broadcast_to(square_root[..., None], (layers_here, heads_here, NOPE)), jnp.broadcast_to(factor[..., None], (layers_here, heads_here, ROPE))], -1)
    rows_q = q_weight.shape[1]
    scaled_q = (q_weight.astype(jnp.float32).reshape(layers_here, rows_q, heads_here, NOPE + ROPE) * column_scale[:, None]).reshape(q_weight.shape).astype(jnp.bfloat16)
    scaled_k = (k_weight.astype(jnp.float32).reshape(layers_here, D_KV, heads_here, NOPE) * square_root[:, None, :, None]).reshape(k_weight.shape).astype(jnp.bfloat16)
    return (scaled_q, scaled_k)

def reference(q_latent, kv_latent, segment_ids, q_weight, k_weight):
    seg_rows = segment_ids.reshape(N_DP, SEQ)
    layer_rows = []
    for layer_idx in range(LAYERS):
        w_query = q_weight[layer_idx]
        w_key = k_weight[layer_idx]

        def one_sequence(inputs):
            latent_q, kv_rows, segments = inputs
            q_full = jnp.dot(latent_q, w_query, preferred_element_type=jnp.float32)
            return sequence_maxima(q_full, kv_rows, segments, w_key)
        per_sequence = lax.map(one_sequence, (q_latent[layer_idx].reshape(N_DP, SEQ, D_Q), kv_latent[layer_idx].reshape(N_DP, SEQ, D_KV + ROPE), seg_rows))
        layer_rows.append(lax.optimization_barrier(jnp.max(per_sequence, axis=0)))
    max_table = jnp.stack(layer_rows)
    scaled_q, scaled_k = scale_weights(max_table, q_weight, k_weight)
    return (max_table / clip_threshold, scaled_q, scaled_k)
```

```python
import functools
import jax
import jax.numpy as jnp
import numpy as np
from jax import lax
from jax.experimental import pallas as pl
from jax.experimental.pallas import tpu as pltpu
from jax.sharding import PartitionSpec as P

D_KV = 512
NOPE = 128
ROPE = 64
HEAD = NOPE + ROPE
LANES = 128
NEG = -1e30
MESH = pl.DeviceIdType.MESH

clip_threshold = 100.0
rope_base = 50000.0


def rotate(values, positions):
    half_width = values.shape[-1] // 2
    frequency = rope_base ** (-jnp.arange(half_width, dtype=jnp.float32) / half_width)
    angles = positions[:, None].astype(jnp.float32) * frequency[None, :]
    cosine = jnp.cos(angles)[:, None, :]
    sine_part = jnp.sin(angles)[:, None, :]
    lower_half = values[..., :half_width]
    upper_half = values[..., half_width:]
    return jnp.concatenate(
        [
            lower_half * cosine - upper_half * sine_part,
            upper_half * cosine + lower_half * sine_part,
        ],
        -1,
    )


def sequence_maxima(q_full, kv_rows, segments, w_key):
    length = kv_rows.shape[0]
    heads_here = w_key.shape[1] // NOPE
    q_full = q_full.reshape(length, heads_here, HEAD)
    positions = jnp.arange(length, dtype=jnp.int32)
    queries = jnp.concatenate(
        [q_full[..., :NOPE], rotate(q_full[..., NOPE:], positions)], -1
    ).astype(jnp.bfloat16)
    key_nope = jnp.dot(kv_rows[:, :D_KV], w_key, preferred_element_type=jnp.float32).astype(
        jnp.bfloat16
    )
    key_nope = key_nope.reshape(length, heads_here, NOPE)
    key_rope = jnp.broadcast_to(kv_rows[:, None, D_KV:], (length, heads_here, ROPE))
    keys_all = jnp.concatenate([key_nope, key_rope], -1)
    logits = jnp.einsum("shd,thd->hst", queries, keys_all, preferred_element_type=jnp.float32)
    logits = logits * HEAD ** (-0.5)
    allowed = (segments[:, None] == segments[None, :]) & (positions[None, :] <= positions[:, None])
    return jnp.max(jnp.where(allowed[None], logits, NEG), axis=(1, 2))


def scale_weights(own_max, q_weight, k_weight):
    factor = clip_threshold / jnp.maximum(own_max, clip_threshold)
    square_root = jnp.sqrt(factor)
    layers, heads = own_max.shape
    q_columns = jnp.concatenate(
        [
            jnp.broadcast_to(square_root[..., None], (layers, heads, NOPE)),
            jnp.broadcast_to(factor[..., None], (layers, heads, ROPE)),
        ],
        -1,
    ).reshape(layers, 1, heads * HEAD)
    k_columns = jnp.broadcast_to(square_root[..., None], (layers, heads, NOPE)).reshape(
        layers, 1, heads * NOPE
    )
    scaled_q = (q_weight.astype(jnp.float32) * q_columns).astype(jnp.bfloat16)
    scaled_k = (k_weight.astype(jnp.float32) * k_columns).astype(jnp.bfloat16)
    return scaled_q, scaled_k


def gathered_maxima(q_latent, kv_latent, segment_ids, q_weight, k_weight):
    q_full = jnp.dot(
        q_latent[0],
        lax.all_gather(q_weight[0], "dp", axis=0, tiled=True),
        preferred_element_type=jnp.float32,
    )
    own_max = sequence_maxima(q_full, kv_latent[0], segment_ids, k_weight[0])[None]
    layer_max = lax.pmax(own_max, "dp")
    return layer_max, lax.all_gather(layer_max, "section", axis=0, tiled=True)


def rope_tables(length):
    half = ROPE // 2
    frequency = np.float32(rope_base) ** (-np.arange(half, dtype=np.float32) / np.float32(half))
    angles = np.arange(length, dtype=np.float32)[:, None] * frequency[None, :].astype(np.float32)
    cosine, sine = np.cos(angles), np.sin(angles)
    zero = np.zeros_like(cosine)
    rest = np.zeros((length, ROPE), np.float32)
    low = [
        np.concatenate([cosine, cosine, rest + 1], 1),
        np.concatenate([-sine, zero, rest], 1),
        np.concatenate([zero, sine, rest], 1),
    ]
    high = [np.roll(t, ROPE, 1) for t in low]
    return np.stack(low + high).astype(np.float32)


def maxima_kernel(
    n_sec, lat_hbm, q_hbm, k_hbm, tab_ref, out_ref,
    lat, wq, wk, keys, bias, macc, tbuf,
    lat_recv, lat_send, w_recv, w_send, k_recv, k_send, t_recv, t_send,
):
    n_seq, length, _ = lat.shape
    rows = q_hbm.shape[0]
    n_pair, d_q, pair = wq.shape
    group_q, group_k = n_pair * pair, wk.shape[1]
    part = length // 2

    z, sec, y = lax.axis_index("dp"), lax.axis_index("section"), lax.axis_index("head")
    c = lax.rem(sec, 2)
    half, z_low = z // 2, lax.rem(z, 2)
    base = sec - c
    primary = c == half
    core_peer = {"section": base + 1 - c}
    y_peer = {"head": 1 - y}
    z_peer = {"dp": 2 * half + 1 - z_low}
    entry = jnp.where(half == 0, 1, 2)
    far = 2 * (1 - half)
    me = z * n_sec + sec

    barrier = pltpu.get_barrier_semaphore()
    for step in range(1, n_seq * n_sec):
        other = lax.rem(me + step, n_seq * n_sec)
        pl.semaphore_signal(
            barrier, inc=1, device_id={"dp": other // n_sec, "section": lax.rem(other, n_sec)},
            device_id_type=MESH,
        )
    pl.semaphore_signal(barrier, inc=1, device_id=y_peer, device_id_type=MESH)

    def local(src, dst, sem):
        return pltpu.make_async_copy(src, dst, sem)

    def ready(dst, sem):
        pltpu.make_async_copy(dst, dst, sem).wait()

    def remote(src, dst, send, recv, where):
        return pltpu.make_async_remote_copy(
            src_ref=src, dst_ref=dst, send_sem=send, recv_sem=recv,
            device_id=where, device_id_type=MESH,
        )

    def lat_at(seq, h):
        return lat.at[seq, pl.ds(h * part, part), :]

    def own_rows(h):
        return lat_hbm.at[pl.ds(h * part, part), :]

    pl.semaphore_wait(barrier, n_seq * n_sec)

    cross_send = remote(own_rows(y), lat_at(z, y), lat_send.at[0], lat_recv.at[z, y], {"dp": 3 - entry})
    near_send = remote(own_rows(y), lat_at(z, y), lat_send.at[0], lat_recv.at[z, y], z_peer)
    core_own = [
        remote(own_rows(h), lat_at(z, h), lat_send.at[1 + h], lat_recv.at[z, h], core_peer)
        for h in range(2)
    ]
    own_group = 2 * z_low + c
    peer_group = 2 * z_low + 1 - c
    k_own = local(k_hbm.at[:, pl.ds(own_group * group_k, group_k)], wk, k_recv)
    k_peer = remote(
        k_hbm.at[:, pl.ds(peer_group * group_k, group_k)], wk, k_send, k_recv, core_peer
    )

    @pl.when(jnp.logical_not(primary))
    def _():
        cross_send.start()

    @pl.when(primary)
    def _():
        near_send.start()
        for h in range(2):
            local(own_rows(h), lat_at(z, h), lat_recv.at[z, h]).start()
            core_own[h].start()
        k_own.start()
        k_peer.start()

    def send_columns(p):
        for j in range(4):
            z_to, c_to = 2 * c + j // 2, j % 2
            src = q_hbm.at[:, pl.ds(j * group_q + p * pair, pair)]
            dst = wq.at[p, pl.ds(z * rows, rows), :]
            mine = (z_to == z) & (c_to == c)

            @pl.when(mine)
            def _():
                local(src, dst, w_recv.at[p, z]).start()

            @pl.when(jnp.logical_not(mine))
            def _():
                remote(
                    src, dst, w_send.at[p, j], w_recv.at[p, z],
                    {"dp": z_to, "section": base + c_to},
                ).start()

    send_columns(0)
    send_columns(1)

    others = [2 * half + 1 - z_low, jnp.where(half == 0, 2, 1), jnp.where(half == 0, 3, 0)]

    def relay(i, seq, h, to_y, to_z):
        slot = lat_at(seq, h)
        sem = lat_recv.at[seq, h]
        out = [remote(slot, slot, lat_send.at[3 + 4 * i + (0 if to_y else 1)], sem, core_peer)]
        if to_y:
            out.append(remote(slot, slot, lat_send.at[3 + 4 * i + 2], sem, y_peer))
        return out, remote(slot, slot, lat_send.at[3 + 4 * i + 3], sem, z_peer)

    at_entry = z == entry

    @pl.when(primary)
    def _():
        for i, seq in enumerate(others):
            first, to_z = relay(i, seq, y, True, i > 0)
            ready(lat_at(seq, y), lat_recv.at[seq, y])
            if i > 0:
                @pl.when(at_entry)
                def _():
                    to_z.start()
            for copy in reversed(first):
                copy.start()
        for i, seq in enumerate(others):
            second, _ = relay(i, seq, 1 - y, False, False)
            ready(lat_at(seq, 1 - y), lat_recv.at[seq, 1 - y])
            second[0].start()
        for h in range(2):
            ready(lat_at(z, h), lat_recv.at[z, h])

    send_columns(2)
    send_columns(3)

    @pl.when(jnp.logical_not(primary))
    def _():
        for seq in range(n_seq):
            for h in range(2):
                ready(lat_at(seq, h), lat_recv.at[seq, h])

    ready(wk, k_recv)

    macc[...] = jnp.full(macc.shape, NEG, jnp.float32)
    lane = lax.broadcasted_iota(jnp.int32, (length, LANES), 1)
    low_lanes = lane < ROPE

    def seq_keys(s, carry):
        tail = lat[s, :, d_q + D_KV:].astype(jnp.float32)
        seg_row = tail.T[ROPE:ROPE + 1, :]
        seg_col = tail[:, ROPE:ROPE + 1]
        row = lax.broadcasted_iota(jnp.int32, (length, length), 0)
        col = lax.broadcasted_iota(jnp.int32, (length, length), 1)
        bias[s] = jnp.where((seg_col == seg_row) & (col <= row), 0.0, NEG)
        rope_low = jnp.where(low_lanes, tail, 0.0)
        rope_high = pltpu.roll(rope_low, ROPE, 1)

        def pair_keys(p, inner):
            columns = pl.ds(pl.multiple_of(p * 2 * NOPE, 2 * NOPE), 2 * NOPE)
            k2 = jnp.dot(
                lat[s, :, d_q:d_q + D_KV], wk[:, columns], preferred_element_type=jnp.float32
            )
            turned = pltpu.roll(k2[:, NOPE:], ROPE, 1)
            keys[s, p, 0, :, :NOPE] = k2[:, :NOPE].astype(jnp.bfloat16)
            keys[s, p, 0, :, NOPE:] = rope_low.astype(jnp.bfloat16)
            keys[s, p, 1, :, :NOPE] = jnp.where(low_lanes, 0.0, turned).astype(jnp.bfloat16)
            keys[s, p, 1, :, NOPE:] = jnp.where(low_lanes, turned, rope_high).astype(jnp.bfloat16)
            return inner

        return lax.fori_loop(0, n_pair, pair_keys, carry)

    lax.fori_loop(0, n_seq, seq_keys, 0)

    def turn(values, at):
        return (
            values * tab_ref[at]
            + pltpu.roll(values, LANES - ROPE // 2, 1) * tab_ref[at + 1]
            + pltpu.roll(values, ROPE // 2, 1) * tab_ref[at + 2]
        ).astype(jnp.bfloat16)

    def pair_logits(p, carry):
        for source in range(n_seq):
            ready(wq.at[p, pl.ds(source * rows, rows), :], w_recv.at[p, source])

        def one(s, inner):
            q2 = jnp.dot(lat[s, :, :d_q], wq[p], preferred_element_type=jnp.float32)
            first = q2[:, :NOPE].astype(jnp.bfloat16)
            middle = turn(q2[:, NOPE:2 * NOPE], 0)
            last = turn(q2[:, 2 * NOPE:], 3)
            for e, tiles in enumerate(((first, middle), (middle, last))):
                queries = jnp.concatenate(tiles, 1)
                for block in range(2):
                    lo, hi = block * part, (block + 1) * part
                    logits = lax.dot_general(
                        queries[lo:hi], keys[s, p, e, :hi, :], (((1,), (1,)), ((), ())),
                        preferred_element_type=jnp.float32,
                    ) + bias[s, lo:hi, :hi]
                    top = jnp.max(logits.reshape(part // 8, 8, hi), axis=0)
                    macc[2 * p + e, :, :hi] = jnp.maximum(macc[2 * p + e, :, :hi], top)
            return inner

        return lax.fori_loop(0, n_seq, one, carry)

    lax.fori_loop(0, n_pair, pair_logits, 0)

    top = jnp.max(jnp.max(macc[...], axis=1), axis=1, keepdims=True) * HEAD ** (-0.5)
    tile = jnp.broadcast_to(top, tbuf.shape)
    tbuf[...] = tile
    out_ref[me] = tile

    def sent(src, sem):
        pltpu.make_async_copy(src, src, sem).wait()

    for p in range(n_pair):
        for j in range(4):
            mine = (2 * c + j // 2 == z) & (j % 2 == c)

            @pl.when(jnp.logical_not(mine))
            def _():
                sent(q_hbm.at[:, pl.ds(j * group_q + p * pair, pair)], w_send.at[p, j])

    @pl.when(jnp.logical_not(primary))
    def _():
        cross_send.wait_send()

    @pl.when(primary)
    def _():
        near_send.wait_send()
        for h in range(2):
            core_own[h].wait_send()
        k_peer.wait_send()
        for i, seq in enumerate(others):
            first, to_z = relay(i, seq, y, True, i > 0)
            for copy in first:
                copy.wait_send()
            if i > 0:
                @pl.when(at_entry)
                def _():
                    to_z.wait_send()
            second, _ = relay(i, seq, 1 - y, False, False)
            second[0].wait_send()

    def table_copy(step):
        other = lax.rem(me + step, n_seq * n_sec)
        return remote(
            tbuf, out_ref.at[me], t_send.at[step], t_recv.at[me],
            {"dp": other // n_sec, "section": lax.rem(other, n_sec)},
        )

    for step in range(1, n_seq * n_sec):
        table_copy(step).start()
    for step in range(1, n_seq * n_sec):
        source = lax.rem(me + step, n_seq * n_sec)
        ready(out_ref.at[source], t_recv.at[source])
    for step in range(1, n_seq * n_sec):
        table_copy(step).wait_send()


def exchanged_maxima(sizes, q_latent, kv_latent, segment_ids, q_weight, k_weight):
    n_dp, n_sec = sizes
    _, length, d_q = q_latent.shape
    rows = q_weight.shape[1]
    heads = k_weight.shape[2] // NOPE
    group = heads // n_dp
    n_pair = group // 2
    width = d_q + D_KV + LANES
    lat = jnp.concatenate(
        [
            q_latent[0],
            kv_latent[0],
            segment_ids[:, None].astype(jnp.bfloat16),
            jnp.zeros((length, LANES - ROPE - 1), jnp.bfloat16),
        ],
        1,
    )
    bf16, dma = jnp.bfloat16, pltpu.SemaphoreType.DMA
    n_all = n_dp * n_sec
    table = pl.pallas_call(
        functools.partial(maxima_kernel, n_sec),
        out_shape=jax.ShapeDtypeStruct((n_all, group, LANES), jnp.float32),
        in_specs=[pl.BlockSpec(memory_space=pltpu.HBM)] * 3
        + [pl.BlockSpec(memory_space=pltpu.VMEM)],
        out_specs=pl.BlockSpec(memory_space=pltpu.VMEM),
        scratch_shapes=[
            pltpu.VMEM((n_dp, length, width), bf16),
            pltpu.VMEM((n_pair, d_q, 2 * HEAD), bf16),
            pltpu.VMEM((D_KV, group * NOPE), bf16),
            pltpu.VMEM((n_dp, n_pair, 2, length, 2 * NOPE), bf16),
            pltpu.VMEM((n_dp, length, length), jnp.float32),
            pltpu.VMEM((group, 8, length), jnp.float32),
            pltpu.VMEM((group, LANES), jnp.float32),
            dma((n_dp, 2)),
            dma((15,)),
            dma((n_pair, n_dp)),
            dma((n_pair, 4)),
            dma,
            dma,
            dma((n_all,)),
            dma((n_all,)),
        ],
        compiler_params=pltpu.CompilerParams(
            collective_id=0, has_side_effects=True, vmem_limit_bytes=60 * 1024 * 1024
        ),
        name="maxima",
    )(lat, q_weight[0], k_weight[0], jnp.asarray(rope_tables(length)))
    by_device = table[:, :, 0].reshape(2, n_dp // 2, n_sec // 2, 2, group)
    max_table = by_device.transpose(2, 0, 1, 3, 4).reshape(n_sec, heads)
    own = lax.dynamic_slice_in_dim(max_table, lax.axis_index("section"), 1, 0)
    return own, max_table


def per_device(sizes, q_latent, kv_latent, segment_ids, q_weight, k_weight):
    n_dp, n_sec, n_head = sizes
    heads = k_weight.shape[2] // NOPE
    length = q_latent.shape[1]
    exchange = (
        n_dp == 4 and n_sec % 2 == 0 and n_head == 2 and heads == 8 * n_dp
        and length % 512 == 0 and q_latent.shape[0] == 1
    )
    args = (q_latent, kv_latent, segment_ids, q_weight, k_weight)
    if exchange:
        own, max_table = exchanged_maxima((n_dp, n_sec), *args)
    else:
        own, max_table = gathered_maxima(*args)
    scaled_q, scaled_k = scale_weights(own, q_weight, k_weight)
    return max_table / clip_threshold, scaled_q, scaled_k


def solution(mesh):
    sizes = tuple(mesh.shape[axis] for axis in ("dp", "section", "head"))
    return jax.shard_map(
        functools.partial(per_device, sizes),
        mesh=mesh,
        in_specs=(
            P("section", "dp", None),
            P("section", "dp", None),
            P("dp"),
            P("section", "dp", "head"),
            P("section", None, "head"),
        ),
        out_specs=(P(None, "head"), P("section", "dp", "head"), P("section", None, "head")),
        check_vma=False,
    )
```

```python
import functools
import jax
import jax.numpy as jnp
import numpy as np
from jax import lax
from jax.experimental import pallas as pl
from jax.experimental.pallas import tpu as pltpu
from jax.sharding import PartitionSpec as P

D_KV = 512
NOPE = 128
ROPE = 64
HEAD = NOPE + ROPE
LANES = 128
NEG = -1e30
VMEM_MIB = 44
MESH = pl.DeviceIdType.MESH

clip_threshold = 100.0
rope_base = 50000.0


def rotate(values, positions):
    half_width = values.shape[-1] // 2
    frequency = rope_base ** (-jnp.arange(half_width, dtype=jnp.float32) / half_width)
    angles = positions[:, None].astype(jnp.float32) * frequency[None, :]
    cosine = jnp.cos(angles)[:, None, :]
    sine_part = jnp.sin(angles)[:, None, :]
    lower_half = values[..., :half_width]
    upper_half = values[..., half_width:]
    return jnp.concatenate(
        [
            lower_half * cosine - upper_half * sine_part,
            upper_half * cosine + lower_half * sine_part,
        ],
        -1,
    )


def sequence_maxima(q_full, kv_rows, segments, w_key):
    length = kv_rows.shape[0]
    heads_here = w_key.shape[1] // NOPE
    q_full = q_full.reshape(length, heads_here, HEAD)
    positions = jnp.arange(length, dtype=jnp.int32)
    queries = jnp.concatenate(
        [q_full[..., :NOPE], rotate(q_full[..., NOPE:], positions)], -1
    ).astype(jnp.bfloat16)
    key_nope = jnp.dot(kv_rows[:, :D_KV], w_key, preferred_element_type=jnp.float32).astype(
        jnp.bfloat16
    )
    key_nope = key_nope.reshape(length, heads_here, NOPE)
    key_rope = jnp.broadcast_to(kv_rows[:, None, D_KV:], (length, heads_here, ROPE))
    keys_all = jnp.concatenate([key_nope, key_rope], -1)
    logits = jnp.einsum("shd,thd->hst", queries, keys_all, preferred_element_type=jnp.float32)
    logits = logits * HEAD ** (-0.5)
    allowed = (segments[:, None] == segments[None, :]) & (positions[None, :] <= positions[:, None])
    return jnp.max(jnp.where(allowed[None], logits, NEG), axis=(1, 2))


def scale_weights(own_max, q_weight, k_weight):
    factor = clip_threshold / jnp.maximum(own_max, clip_threshold)
    square_root = jnp.sqrt(factor)
    layers, heads = own_max.shape
    q_columns = jnp.concatenate(
        [
            jnp.broadcast_to(square_root[..., None], (layers, heads, NOPE)),
            jnp.broadcast_to(factor[..., None], (layers, heads, ROPE)),
        ],
        -1,
    ).reshape(layers, 1, heads * HEAD)
    k_columns = jnp.broadcast_to(square_root[..., None], (layers, heads, NOPE)).reshape(
        layers, 1, heads * NOPE
    )
    scaled_q = (q_weight.astype(jnp.float32) * q_columns).astype(jnp.bfloat16)
    scaled_k = (k_weight.astype(jnp.float32) * k_columns).astype(jnp.bfloat16)
    return scaled_q, scaled_k


def gathered_maxima(q_latent, kv_latent, segment_ids, q_weight, k_weight):
    q_full = jnp.dot(
        q_latent[0],
        lax.all_gather(q_weight[0], "dp", axis=0, tiled=True),
        preferred_element_type=jnp.float32,
    )
    own_max = sequence_maxima(q_full, kv_latent[0], segment_ids, k_weight[0])[None]
    layer_max = lax.pmax(own_max, "dp")
    return layer_max, lax.all_gather(layer_max, "section", axis=0, tiled=True)


def rope_tables(length):
    half = ROPE // 2
    frequency = np.float32(rope_base) ** (-np.arange(half, dtype=np.float32) / np.float32(half))
    angles = np.arange(length, dtype=np.float32)[:, None] * frequency[None, :].astype(np.float32)
    cosine, sine = np.cos(angles), np.sin(angles)
    zero = np.zeros_like(cosine)
    rest = np.zeros((length, ROPE), np.float32)
    low = [
        np.concatenate([cosine, cosine, rest + 1], 1),
        np.concatenate([-sine, zero, rest], 1),
        np.concatenate([zero, sine, rest], 1),
    ]
    high = [np.roll(t, ROPE, 1) for t in low]
    return np.stack(low + high).astype(np.float32)


def maxima_kernel(
    n_sec, x_hbm, kv_hbm, seg_hbm, q_hbm, k_hbm, tab_ref, out_ref,
    lat, kvt, seg, wq, wk, keys, bias, macc, tbuf,
    lat_recv, lat_send, seg_recv, seg_send, w_recv, w_send, k_recv, k_send, t_recv, t_send,
):
    n_seq, length, _ = lat.shape
    rows = q_hbm.shape[0]
    n_pair, d_q, pair = wq.shape
    group_q, group_k = n_pair * pair, wk.shape[1]
    part = length // 2

    z, sec, y = lax.axis_index("dp"), lax.axis_index("section"), lax.axis_index("head")
    c = lax.rem(sec, 2)
    half, z_low = z // 2, lax.rem(z, 2)
    base = sec - c
    primary = c == half
    core_peer = {"section": base + 1 - c}
    y_peer = {"head": 1 - y}
    z_peer = {"dp": 2 * half + 1 - z_low}
    entry = jnp.where(half == 0, 1, 2)
    me = z * n_sec + sec

    barrier = pltpu.get_barrier_semaphore()
    for step in range(1, n_seq * n_sec):
        other = lax.rem(me + step, n_seq * n_sec)
        pl.semaphore_signal(
            barrier, inc=1, device_id={"dp": other // n_sec, "section": lax.rem(other, n_sec)},
            device_id_type=MESH,
        )
    pl.semaphore_signal(barrier, inc=1, device_id=y_peer, device_id_type=MESH)

    def local(src, dst, sem):
        return pltpu.make_async_copy(src, dst, sem)

    def ready(dst, sem):
        pltpu.make_async_copy(dst, dst, sem).wait()

    def remote(src, dst, send, recv, where):
        return pltpu.make_async_remote_copy(
            src_ref=src, dst_ref=dst, send_sem=send, recv_sem=recv,
            device_id=where, device_id_type=MESH,
        )

    def slots(seq, h):
        at = pl.ds(pl.multiple_of(h * part, part), part)
        return lat.at[seq, at, :], kvt.at[seq, :, at]

    def own(h):
        at = pl.ds(pl.multiple_of(h * part, part), part)
        return x_hbm.at[at, :], kv_hbm.at[:, at]

    def send(sources, seq, h, at, where, do):
        for i, (src, dst) in enumerate(zip(sources, slots(seq, h))):
            getattr(
                remote(src, dst, lat_send.at[at, i], lat_recv.at[seq, h, i], where), do
            )()

    def ready_half(seq, h):
        for i, dst in enumerate(slots(seq, h)):
            ready(dst, lat_recv.at[seq, h, i])

    own_group = 2 * z_low + c
    peer_group = 2 * z_low + 1 - c

    def group_columns(g):
        return k_hbm.at[:, pl.ds(pl.multiple_of(g * group_k, group_k), group_k)]

    def seg_copy(step):
        return remote(
            seg_hbm, seg.at[z], seg_send.at[step], seg_recv.at[z],
            {"dp": lax.rem(z + step, n_seq)},
        )

    def own_sends(do):
        for step in range(1, n_seq):
            getattr(seg_copy(step), do)()

        @pl.when(jnp.logical_not(primary))
        def _():
            send(own(y), z, y, 0, {"dp": 3 - entry}, do)

        @pl.when(primary)
        def _():
            send(own(y), z, y, 0, z_peer, do)
            for h in range(2):
                send(own(h), z, h, 1 + h, core_peer, do)
            k_peer = remote(group_columns(peer_group), wk, k_send, k_recv, core_peer)
            getattr(k_peer, do)()

    def columns(p, j, act):
        turn_to = lax.rem(j + 2 * z_low, 4)
        z_to, c_to = 2 * c + turn_to // 2, lax.rem(turn_to, 2)
        offset = pl.multiple_of(turn_to * group_q + p * pair, LANES)
        src = q_hbm.at[:, pl.ds(offset, pair)]
        dst = wq.at[p, pl.ds(pl.multiple_of(z * rows, rows), rows), :]
        mine = (z_to == z) & (c_to == c)
        there = {"dp": z_to, "section": base + c_to}
        if act == "start":
            @pl.when(mine)
            def _():
                local(src, dst, w_recv.at[p, z]).start()

        @pl.when(jnp.logical_not(mine))
        def _():
            getattr(remote(src, dst, w_send.at[p, j], w_recv.at[p, z], there), act)()

    def send_columns(p):
        for j in range(4):
            columns(p, j, "start")

    pl.semaphore_wait(barrier, n_seq * n_sec)

    own_sends("start")
    local(seg_hbm, seg.at[z], seg_recv.at[z]).start()

    @pl.when(primary)
    def _():
        for h in range(2):
            for i, (src, dst) in enumerate(zip(own(h), slots(z, h))):
                local(src, dst, lat_recv.at[z, h, i]).start()
        local(group_columns(own_group), wk, k_recv).start()

    send_columns(0)
    send_columns(1)

    others = [2 * half + 1 - z_low, jnp.where(half == 0, 2, 1), jnp.where(half == 0, 3, 0)]
    at_entry = z == entry

    def relay_first(i, seq, do):
        if i > 0:
            @pl.when(at_entry)
            def _():
                send(slots(seq, y), seq, y, 6 + 4 * i, z_peer, do)
        send(slots(seq, y), seq, y, 5 + 4 * i, y_peer, do)
        send(slots(seq, y), seq, y, 3 + 4 * i, core_peer, do)

    def relay_second(i, seq, do):
        send(slots(seq, 1 - y), seq, 1 - y, 4 + 4 * i, core_peer, do)

    @pl.when(primary)
    def _():
        for i, seq in enumerate(others):
            ready_half(seq, y)
            relay_first(i, seq, "start")
        for i, seq in enumerate(others):
            ready_half(seq, 1 - y)
            relay_second(i, seq, "start")
        for h in range(2):
            ready_half(z, h)

    send_columns(2)
    send_columns(3)

    @pl.when(jnp.logical_not(primary))
    def _():
        for seq in range(n_seq):
            for h in range(2):
                ready_half(seq, h)

    ready(wk, k_recv)
    for seq in range(n_seq):
        ready(seg.at[seq], seg_recv.at[seq])

    macc[...] = jnp.full(macc.shape, NEG, jnp.float32)

    def seq_keys(s, carry):
        seg_row = seg[s].astype(jnp.float32)
        seg_col = jnp.broadcast_to(seg_row, (LANES, length)).T[:, :1]
        row = lax.broadcasted_iota(jnp.int32, (length, length), 0)
        col = lax.broadcasted_iota(jnp.int32, (length, length), 1)
        bias[s] = jnp.where((seg_col == seg_row) & (col <= row), 0.0, NEG)
        rope = kvt[s, D_KV:, :]
        none = jnp.zeros((ROPE, length), jnp.bfloat16)
        for p in range(n_pair):
            k2 = lax.dot_general(
                wk[:, p * 2 * NOPE:(p + 1) * 2 * NOPE], kvt[s, :D_KV, :],
                (((0,), (0,)), ((), ())), preferred_element_type=jnp.float32,
            ).astype(jnp.bfloat16)
            keys[s, p, 0, :NOPE, :] = k2[:NOPE]
            keys[s, p, 0, NOPE:HEAD, :] = rope
            keys[s, p, 0, HEAD:, :] = none
            keys[s, p, 1, :ROPE, :] = none
            keys[s, p, 1, ROPE:HEAD, :] = k2[NOPE:]
            keys[s, p, 1, HEAD:, :] = rope
        return carry

    lax.fori_loop(0, n_seq, seq_keys, 0)

    def turn(values, at):
        return (
            values * tab_ref[at]
            + pltpu.roll(values, LANES - ROPE // 2, 1) * tab_ref[at + 1]
            + pltpu.roll(values, ROPE // 2, 1) * tab_ref[at + 2]
        ).astype(jnp.bfloat16)

    def pair_logits(p, carry):
        for source in range(n_seq):
            ready(wq.at[p, pl.ds(source * rows, rows), :], w_recv.at[p, source])

        def one(s, inner):
            q2 = jnp.dot(lat[s], wq[p], preferred_element_type=jnp.float32)
            first = q2[:, :NOPE].astype(jnp.bfloat16)
            middle = turn(q2[:, NOPE:2 * NOPE], 0)
            last = turn(q2[:, 2 * NOPE:], 3)
            for e, tiles in enumerate(((first, middle), (middle, last))):
                queries = jnp.concatenate(tiles, 1)
                for block in range(2):
                    lo, hi = block * part, (block + 1) * part
                    logits = jnp.dot(
                        queries[lo:hi], keys[s, p, e, :, :hi], preferred_element_type=jnp.float32
                    ) + bias[s, lo:hi, :hi]
                    top = jnp.max(logits.reshape(part // 8, 8, hi), axis=0)
                    macc[2 * p + e, :, :hi] = jnp.maximum(macc[2 * p + e, :, :hi], top)
            return inner

        return lax.fori_loop(0, n_seq, one, carry)

    lax.fori_loop(0, n_pair, pair_logits, 0)

    top = jnp.max(jnp.max(macc[...], axis=1), axis=1, keepdims=True) * HEAD ** (-0.5)
    tile = jnp.broadcast_to(top, tbuf.shape)
    tbuf[...] = tile
    out_ref[me] = tile

    for p in range(n_pair):
        for j in range(4):
            columns(p, j, "wait_send")
    own_sends("wait_send")

    @pl.when(primary)
    def _():
        for i, seq in enumerate(others):
            relay_first(i, seq, "wait_send")
            relay_second(i, seq, "wait_send")

    def table_copy(step):
        other = lax.rem(me + step, n_seq * n_sec)
        return remote(
            tbuf, out_ref.at[me], t_send.at[step], t_recv.at[me],
            {"dp": other // n_sec, "section": lax.rem(other, n_sec)},
        )

    for step in range(1, n_seq * n_sec):
        table_copy(step).start()
    for step in range(1, n_seq * n_sec):
        source = lax.rem(me + step, n_seq * n_sec)
        ready(out_ref.at[source], t_recv.at[source])
    for step in range(1, n_seq * n_sec):
        table_copy(step).wait_send()


def scale_kernel(n_sec, table, q_ref, k_ref, ratio_ref, q_out, k_out):
    n_group = pl.num_programs(0)
    g = pl.program_id(0)
    sec = lax.axis_index("section")
    group = table.shape[1]

    def slot(layer, number):
        z_of = 2 * lax.rem(layer, 2) + number // 2
        return z_of * n_sec + 2 * (layer // 2) + lax.rem(number, 2)

    factor = clip_threshold / jnp.maximum(table[slot(sec, g)], clip_threshold)
    root = jnp.sqrt(factor)
    low = lax.broadcasted_iota(jnp.int32, (1, LANES), 1) < ROPE
    for p in range(group // 2):
        f_a, f_b = factor[2 * p:2 * p + 1], factor[2 * p + 1:2 * p + 2]
        r_a, r_b = root[2 * p:2 * p + 1], root[2 * p + 1:2 * p + 2]
        scales = (r_a, jnp.where(low, f_a, r_b), jnp.where(low, r_b, f_b))
        for i, scale in enumerate(scales):
            at = pl.ds(p * 2 * HEAD + i * LANES, LANES)
            q_out[:, at] = (q_ref[:, at].astype(jnp.float32) * scale).astype(jnp.bfloat16)
        for i, scale in enumerate((r_a, r_b)):
            at = pl.ds((2 * p + i) * NOPE, NOPE)
            k_out[:, at] = (k_ref[:, at].astype(jnp.float32) * scale).astype(jnp.bfloat16)

    @pl.when(g == 0)
    def _():
        lane = lax.broadcasted_iota(jnp.int32, (group, LANES), 1)
        place = lax.broadcasted_iota(jnp.int32, (group, LANES), 0)
        for layer in range(ratio_ref.shape[0]):
            line = jnp.zeros((1, LANES), jnp.float32)
            for number in range(ratio_ref.shape[1] // group):
                z_of = 2 * (layer % 2) + number // 2
                values = table[z_of * n_sec + 2 * (layer // 2) + number % 2]
                here = lane == number * group + place
                line = line + jnp.sum(jnp.where(here, values, 0.0), axis=0, keepdims=True)
            ratio_ref[layer:layer + 1, :] = line[:, :ratio_ref.shape[1]] / clip_threshold


def exchanged(sizes, q_latent, kv_latent, segment_ids, q_weight, k_weight):
    n_dp, n_sec = sizes
    _, length, d_q = q_latent.shape
    rows = q_weight.shape[1]
    heads = k_weight.shape[2] // NOPE
    group = heads // n_dp
    n_pair = group // 2
    bf16, dma = jnp.bfloat16, pltpu.SemaphoreType.DMA
    n_all = n_dp * n_sec
    table = pl.pallas_call(
        functools.partial(maxima_kernel, n_sec),
        out_shape=jax.ShapeDtypeStruct((n_all, group, LANES), jnp.float32),
        in_specs=[pl.BlockSpec(memory_space=pltpu.HBM)] * 5
        + [pl.BlockSpec(memory_space=pltpu.VMEM)],
        out_specs=pl.BlockSpec(memory_space=pltpu.VMEM),
        scratch_shapes=[
            pltpu.VMEM((n_dp, length, d_q), bf16),
            pltpu.VMEM((n_dp, D_KV + ROPE, length), bf16),
            pltpu.VMEM((n_dp, 1, length), jnp.int32),
            pltpu.VMEM((n_pair, d_q, 2 * HEAD), bf16),
            pltpu.VMEM((D_KV, group * NOPE), bf16),
            pltpu.VMEM((n_dp, n_pair, 2, 2 * NOPE, length), bf16),
            pltpu.VMEM((n_dp, length, length), jnp.float32),
            pltpu.VMEM((group, 8, length), jnp.float32),
            pltpu.VMEM((group, LANES), jnp.float32),
            dma((n_dp, 2, 2)),
            dma((15, 2)),
            dma((n_dp,)),
            dma((n_dp,)),
            dma((n_pair, n_dp)),
            dma((n_pair, 4)),
            dma,
            dma,
            dma((n_all,)),
            dma((n_all,)),
        ],
        compiler_params=pltpu.CompilerParams(
            collective_id=0, has_side_effects=True, vmem_limit_bytes=VMEM_MIB * 1024 * 1024
        ),
        cost_estimate=pl.CostEstimate(
            flops=2 * n_dp * length * group * (HEAD * (d_q + length) + NOPE * D_KV),
            bytes_accessed=2 * rows * heads * HEAD, transcendentals=0,
        ),
        name="maxima",
    )(
        q_latent[0], kv_latent[0].T, segment_ids.reshape(1, length), q_weight[0], k_weight[0],
        jnp.asarray(rope_tables(length)),
    )
    ratio, scaled_q, scaled_k = pl.pallas_call(
        functools.partial(scale_kernel, n_sec),
        grid=(n_dp,),
        out_shape=(
            jax.ShapeDtypeStruct((n_sec, heads), jnp.float32),
            jax.ShapeDtypeStruct(q_weight.shape[1:], bf16),
            jax.ShapeDtypeStruct(k_weight.shape[1:], bf16),
        ),
        in_specs=[
            pl.BlockSpec((n_all, group, LANES), lambda g: (0, 0, 0)),
            pl.BlockSpec((rows, group * HEAD), lambda g: (0, g)),
            pl.BlockSpec((D_KV, group * NOPE), lambda g: (0, g)),
        ],
        out_specs=[
            pl.BlockSpec((n_sec, heads), lambda g: (0, 0)),
            pl.BlockSpec((rows, group * HEAD), lambda g: (0, g)),
            pl.BlockSpec((D_KV, group * NOPE), lambda g: (0, g)),
        ],
        compiler_params=pltpu.CompilerParams(
            dimension_semantics=("arbitrary",), vmem_limit_bytes=24 * 1024 * 1024
        ),
        cost_estimate=pl.CostEstimate(
            flops=rows * heads * HEAD, bytes_accessed=8 * rows * heads * HEAD, transcendentals=0
        ),
        name="scale",
    )(table, q_weight[0], k_weight[0])
    return ratio, scaled_q[None], scaled_k[None]


def per_device(sizes, q_latent, kv_latent, segment_ids, q_weight, k_weight):
    n_dp, n_sec, n_head = sizes
    heads = k_weight.shape[2] // NOPE
    length = q_latent.shape[1]
    exchange = (
        n_dp == 4 and n_sec % 2 == 0 and q_weight.shape[1] % 8 == 0 and n_head == 2 and heads == 8 * n_dp
        and length % 512 == 0 and q_latent.shape[0] == 1
    )
    args = (q_latent, kv_latent, segment_ids, q_weight, k_weight)
    if exchange:
        return exchanged((n_dp, n_sec), *args)
    own, max_table = gathered_maxima(*args)
    scaled_q, scaled_k = scale_weights(own, q_weight, k_weight)
    return max_table / clip_threshold, scaled_q, scaled_k


def solution(mesh):
    sizes = tuple(mesh.shape[axis] for axis in ("dp", "section", "head"))
    return jax.shard_map(
        functools.partial(per_device, sizes),
        mesh=mesh,
        in_specs=(
            P("section", "dp", None),
            P("section", "dp", None),
            P("dp"),
            P("section", "dp", "head"),
            P("section", None, "head"),
        ),
        out_specs=(P(None, "head"), P("section", "dp", "head"), P("section", None, "head")),
        check_vma=False,
    )
```
